32 devices in a mesh: gx: 4 (over y, x), gy: 8 (over z, core).
Axes of the slice: x: 2, y: 2, z: 4, core: 2. Of those that a mesh axis runs over, the one named last changes fastest.
Arguments:
- tokens: bfloat16 [4096, 8192], P('gy', 'gx'), may hold values from -6 to 6
- pair_ids: int32 [8], replicated, may hold values from 0 to 7, each once
- query_weight: bfloat16 [8192, 8192], P('gy', 'gx'), may hold values from -0.0625 to 0.0625
- key_matrix: bfloat16 [8192, 1024], P('gy', 'gx'), may hold values from -0.0625 to 0.0625
- value_matrix: bfloat16 [8192, 1024], P('gy', 'gx'), may hold values from -0.0625 to 0.0625
- query_bias: bfloat16 [8192], P('gx'), may hold values from -13 to 13
- key_bias: bfloat16 [1024], P('gx'), may hold values from -8 to 8
- value_offset_bias: bfloat16 [1024], P('gx'), may hold values from -3 to 3
Outputs:
- attn_out: bfloat16 [4096, 8192], P('gy', 'gx')
The draws below stay inside these ranges and needn't reach their ends.
Inputs may be any that keep to these rules, and one draw needn't show every extreme that they name: `pair_ids`: each number from 0 to 7 appears once.
All inputs are finite; a program needn't handle non-finite values.
Results may differ from the reference program's by a relative error of at most 0.0055.
The reference program's roundings to bfloat16 on the way count: a program that leaves them out, or rounds other values in their place, can miss the bound.
Values may be sent and summed in bfloat16 or wider, within the bound.
A program may use at most 128 MiB of HBM per device.

```python
import math
import jax
import jax.numpy as jnp
from jax import lax

MODEL_WIDTH = 8192
QUERY_HEADS = 64
KEY_VALUE_HEADS = 8
HEAD_SIZE = 128
TOK_DEV = 512
SEQ = 4096


def draw_query_bias(key, part):
    random_jitter = jnp.clip(0.5 * jax.random.normal(jax.random.fold_in(key, 11), (QUERY_HEADS, HEAD_SIZE), jnp.float32), -3.0, 3.0)
    return random_jitter.reshape(QUERY_HEADS * HEAD_SIZE).astype(jnp.bfloat16)


def draw_key_bias(key, part):
    random_jitter = jnp.clip(0.5 * jax.random.normal(jax.random.fold_in(key, 21), (KEY_VALUE_HEADS, HEAD_SIZE), jnp.float32), -3.0, 3.0)
    return random_jitter.reshape(KEY_VALUE_HEADS * HEAD_SIZE).astype(jnp.bfloat16)


def steps_of(rng, dims, pieces, smallest, top_value):
    def one(dim, parts):
        heights = jax.random.uniform(jax.random.fold_in(jax.random.fold_in(rng, 6), dim), (parts,), jnp.float32, smallest / len(pieces), top_value / len(pieces))
        return jnp.repeat(jnp.exp(heights), dims[dim] // parts).reshape((-1,) + (1,) * (len(dims) - dim - 1))

    level = one(*pieces[0])
    for cut in pieces[1:]:
        level = level * one(*cut)
    return level


def centred(rng, extent, scale, bound, cuts=(), kind=jnp.bfloat16):
    loudness = steps_of(rng, extent, cuts, -0.22, 0.18) if cuts else 1.0
    array = jax.random.normal(rng, extent, jnp.float32) * scale * loudness
    return jnp.minimum(jnp.maximum(array, -bound), bound).astype(kind)


def setup_inputs(seed: int = 0) -> dict:
    keys = jax.random.split(jax.random.key(seed), 9)
    tokens = centred(keys[0], (SEQ, MODEL_WIDTH), 1.0, 6.0, ((0, 8), (1, 4)))
    pair_ids = jax.random.permutation(keys[1], SEQ // TOK_DEV).astype(jnp.int32)
    query_weight = centred(keys[2], (MODEL_WIDTH, QUERY_HEADS * HEAD_SIZE), MODEL_WIDTH ** -0.5, 0.0625, ((0, 8), (1, 4)))
    key_matrix = centred(keys[3], (MODEL_WIDTH, KEY_VALUE_HEADS * HEAD_SIZE), MODEL_WIDTH ** -0.5, 0.0625, ((0, 8), (1, 4)))
    value_matrix = centred(keys[4], (MODEL_WIDTH, KEY_VALUE_HEADS * HEAD_SIZE), MODEL_WIDTH ** -0.5, 0.0625, ((0, 8), (1, 4)))
    query_bias = draw_query_bias(jax.random.fold_in(keys[8], 71), 0)
    key_bias = draw_key_bias(jax.random.fold_in(keys[8], 71), 0)
    value_offset_bias = centred(keys[7], (KEY_VALUE_HEADS * HEAD_SIZE,), 0.5, 3.0, ((0, 4),))
    return {"tokens": tokens, "pair_ids": pair_ids, "query_weight": query_weight, "key_matrix": key_matrix, "value_matrix": value_matrix, "query_bias": query_bias, "key_bias": key_bias, "value_offset_bias": value_offset_bias}


rope_theta = 1000000.0
neg_large = -1e+30

def table_lookup(entries, wanted):
    slot_ids = lax.iota(jnp.int32, entries.shape[0])
    return lax.optimization_barrier(jnp.sum(jnp.where(wanted[:, None] == slot_ids[None, :], entries[None, :], 0), axis=1)).astype(jnp.int32)

def layout_positions(pair_ids, total_row_count, tok_dev):
    half_len = tok_dev // 2
    row_ids = lax.iota(jnp.int32, total_row_count)
    within = row_ids % tok_dev
    owners = table_lookup(pair_ids, row_ids // tok_dev)
    mirrored = 2 * pair_ids.shape[0] - 1 - owners
    return jnp.where(within < half_len, owners * half_len + within, mirrored * half_len + within - half_len).astype(jnp.int32)

def apply_rotary(values, token_positions):
    half_size = values.shape[-1] // 2
    frequency = jnp.exp(lax.iota(jnp.float32, half_size) * (-2.0 * math.log(rope_theta) / values.shape[-1]))
    angles = token_positions.astype(jnp.float32)[:, None] * frequency[None, :]
    cos_part = jnp.cos(angles)[:, None, :]
    sin_part = jnp.sin(angles)[:, None, :]
    lower_half = values[..., :half_size]
    upper_half = values[..., half_size:]
    return jnp.concatenate([lower_half * cos_part - upper_half * sin_part, upper_half * cos_part + lower_half * sin_part], axis=-1)

def reference(tokens, pair_ids, query_weight, key_matrix, value_matrix, query_bias, key_bias, value_offset_bias):
    total_row_count = tokens.shape[0]
    token_positions = layout_positions(pair_ids, total_row_count, TOK_DEV)
    queries = jnp.dot(tokens, query_weight, preferred_element_type=jnp.float32) + query_bias.astype(jnp.float32)
    queries = apply_rotary(queries.reshape(total_row_count, QUERY_HEADS, HEAD_SIZE), token_positions).astype(jnp.bfloat16)
    projected_key_rows = jnp.dot(tokens, key_matrix, preferred_element_type=jnp.float32) + key_bias.astype(jnp.float32)
    projected_key_rows = apply_rotary(projected_key_rows.reshape(total_row_count, KEY_VALUE_HEADS, HEAD_SIZE), token_positions).astype(jnp.bfloat16)
    projected_value_rows = (jnp.dot(tokens, value_matrix, preferred_element_type=jnp.float32) + value_offset_bias.astype(jnp.float32)).astype(jnp.bfloat16)
    projected_value_rows = projected_value_rows.reshape(total_row_count, KEY_VALUE_HEADS, HEAD_SIZE)
    visible = token_positions[None, :] <= token_positions[:, None]
    query_group_width = QUERY_HEADS // KEY_VALUE_HEADS
    scale = 1.0 / math.sqrt(HEAD_SIZE)

    def one_head(head_id):
        query_head = lax.dynamic_index_in_dim(queries, head_id, 1, keepdims=False)
        kv_head = head_id // query_group_width
        key_head = lax.dynamic_index_in_dim(projected_key_rows, kv_head, 1, keepdims=False)
        value_head = lax.dynamic_index_in_dim(projected_value_rows, kv_head, 1, keepdims=False)
        scores = jnp.dot(query_head, key_head.T, preferred_element_type=jnp.float32) * scale
        scores = jnp.where(visible, scores, neg_large)
        row_peak = lax.optimization_barrier(jnp.max(scores, axis=-1))
        probs = jnp.where(visible, jnp.exp(scores - row_peak[:, None]), 0.0)
        totals = lax.optimization_barrier(jnp.sum(probs, axis=-1))
        mixed = jnp.dot(probs.astype(jnp.bfloat16), value_head, preferred_element_type=jnp.float32)
        return (mixed / totals[:, None]).astype(jnp.bfloat16)
    outputs = lax.map(one_head, jnp.arange(QUERY_HEADS, dtype=jnp.int32))
    return outputs.transpose(1, 0, 2).reshape(total_row_count, QUERY_HEADS * HEAD_SIZE)
```

```python
import math

import jax
import jax.numpy as jnp
from jax import lax
from jax.experimental import pallas as pl
from jax.experimental.pallas import tpu as pltpu
from jax.sharding import PartitionSpec as P

HEAD_SIZE = 128


rope_theta = 1000000.0
neg_large = -1e30


def table_lookup(entries, wanted):
    slot_ids = lax.iota(jnp.int32, entries.shape[0])
    return jnp.sum(jnp.where(wanted[:, None] == slot_ids[None, :], entries[None, :], 0), axis=1)


def layout_positions(pair_ids, total_row_count, tok_dev):
    half_len = tok_dev // 2
    row_ids = lax.iota(jnp.int32, total_row_count)
    within = row_ids % tok_dev
    owners = table_lookup(pair_ids, row_ids // tok_dev)
    mirrored = 2 * pair_ids.shape[0] - 1 - owners
    return jnp.where(
        within < half_len, owners * half_len + within, mirrored * half_len + within - half_len
    )


def apply_rotary(values, token_positions):
    half_size = values.shape[-1] // 2
    frequency = jnp.exp(
        lax.iota(jnp.float32, half_size) * (-2.0 * math.log(rope_theta) / values.shape[-1])
    )
    angles = token_positions.astype(jnp.float32)[:, None] * frequency[None, :]
    cos_part = jnp.cos(angles)[:, None, :]
    sin_part = jnp.sin(angles)[:, None, :]
    lower_half = values[..., :half_size]
    upper_half = values[..., half_size:]
    return jnp.concatenate(
        [
            lower_half * cos_part - upper_half * sin_part,
            upper_half * cos_part + lower_half * sin_part,
        ],
        axis=-1,
    )


def attend(order_ref, own_ref, q_ref, cos_ref, sin_ref, k_ref, v_ref, o_ref, q_s, acc, peak, total):
    half_len = cos_ref.shape[0]
    heads = q_ref.shape[1] // HEAD_SIZE
    factor = math.log2(math.e) / math.sqrt(HEAD_SIZE)
    side = pl.program_id(0)
    own = own_ref[0]
    count = jnp.where(side == 0, own, own_ref[1])
    cos_part = cos_ref[...]
    sin_part = sin_ref[...]
    for h in range(heads):
        x = q_ref[:, h * HEAD_SIZE : (h + 1) * HEAD_SIZE]
        turned = x * cos_part + pltpu.roll(x, HEAD_SIZE // 2, 1) * sin_part
        q_s[h] = turned.astype(jnp.bfloat16)

    def scores(h, slot):
        return lax.dot_general(
            k_ref[slot], q_s[h], (((1,), (1,)), ((), ())), preferred_element_type=jnp.float32
        )

    slot = order_ref[count]
    keep = lax.broadcasted_iota(jnp.int32, (half_len, half_len), 0) <= lax.broadcasted_iota(
        jnp.int32, (half_len, half_len), 1
    )
    for h in range(heads):
        s = jnp.where(keep, scores(h, slot), neg_large)
        top = jnp.max(s, axis=0, keepdims=True)
        p = jnp.where(keep, jnp.exp2((s - top) * factor), 0.0)
        peak[h] = top
        total[h] = jnp.sum(p, axis=0, keepdims=True)
        acc[h] = jnp.dot(v_ref[slot], p.astype(jnp.bfloat16), preferred_element_type=jnp.float32)

    @pl.loop(0, count)
    def _(j):
        place = order_ref[j]
        for h in range(heads):
            s = scores(h, place)
            before = peak[h]
            top = jnp.maximum(before, jnp.max(s, axis=0, keepdims=True))
            p = jnp.exp2((s - top) * factor)
            shrink = jnp.exp2((before - top) * factor)
            peak[h] = top
            total[h] = total[h] * shrink + jnp.sum(p, axis=0, keepdims=True)
            acc[h] = acc[h] * shrink + jnp.dot(
                v_ref[place], p.astype(jnp.bfloat16), preferred_element_type=jnp.float32
            )

    for h in range(heads):
        o_ref[:, h * HEAD_SIZE : (h + 1) * HEAD_SIZE] = (
            (acc[h] / total[h]).T.astype(o_ref.dtype)
        )


def group_attention(order, own, q, cos_full, sin_full, k, v):
    rows, width = q.shape
    half_len = rows // 2
    heads = width // HEAD_SIZE
    block = heads // 2 if heads % 2 == 0 else heads
    slots = k.shape[0]
    flops = rows * width * 4 * (slots + 1) * half_len // 2
    return pl.pallas_call(
        attend,
        grid_spec=pltpu.PrefetchScalarGridSpec(
            num_scalar_prefetch=2,
            grid=(2, heads // block),
            in_specs=[
                pl.BlockSpec((half_len, block * HEAD_SIZE), lambda i, j, *_: (i, j)),
                pl.BlockSpec((half_len, HEAD_SIZE), lambda i, j, *_: (i, 0)),
                pl.BlockSpec((half_len, HEAD_SIZE), lambda i, j, *_: (i, 0)),
                pl.BlockSpec(k.shape, lambda i, j, *_: (0, 0, 0)),
                pl.BlockSpec(v.shape, lambda i, j, *_: (0, 0, 0)),
            ],
            out_specs=pl.BlockSpec((half_len, block * HEAD_SIZE), lambda i, j, *_: (i, j)),
            scratch_shapes=[
                pltpu.VMEM((block, half_len, HEAD_SIZE), jnp.bfloat16),
                pltpu.VMEM((block, HEAD_SIZE, half_len), jnp.float32),
                pltpu.VMEM((block, 1, half_len), jnp.float32),
                pltpu.VMEM((block, 1, half_len), jnp.float32),
            ],
        ),
        out_shape=jax.ShapeDtypeStruct((rows, width), jnp.bfloat16),
        compiler_params=pltpu.CompilerParams(vmem_limit_bytes=32 * 1024 * 1024),
        cost_estimate=pl.CostEstimate(
            flops=flops, bytes_accessed=8 * rows * width, transcendentals=flops // (4 * HEAD_SIZE)
        ),
    )(order, own, q, cos_full, sin_full, k, v)


def ring_pieces(block):
    size = lax.axis_size("gy")
    me = lax.axis_index("gy")
    chips = size // 2
    rows = block.shape[0]

    def move(x, step):
        return lax.ppermute(x, "gy", [(i, (i + step) % size) for i in range(size)])

    mine = [(me, 0, block)]
    ahead = behind = block
    first = []
    for d in range(1, chips // 2 + 1):
        if 2 * d == chips and chips > 2:
            ahead, behind = ahead[: rows // 2], behind[rows // 2 :]
        elif 2 * d == chips:
            ahead, behind = ahead[: rows // 2], behind[rows // 2 :]
        ahead = move(ahead, 2)
        behind = move(behind, -2)
        if d == 1:
            first = [ahead, behind]
        mine.append(((me - 2 * d) % size, 0, ahead))
        mine.append(((me + 2 * d) % size, rows // 2 if 2 * d == chips else 0, behind))
    swap = [(i, i ^ 1) for i in range(size)]
    other = [
        (owner + 1 - 2 * (owner % 2), start, lax.ppermute(x, "gy", swap))
        for owner, start, x in mine
    ]
    return mine + other, first


def project(gathered, pieces, rows, bias):
    total = None
    for owner, start, x in pieces:
        part = lax.dynamic_slice_in_dim(gathered, owner * rows + start, x.shape[0], 1)
        term = jnp.dot(part, x, preferred_element_type=jnp.float32)
        total = term if total is None else total + term
    return total + bias.astype(jnp.float32)


def on_device(
    tokens,
    pair_ids,
    query_weight,
    key_matrix,
    value_matrix,
    query_bias,
    key_bias,
    value_offset_bias,
):
    tok_dev = tokens.shape[0]
    half_len = tok_dev // 2
    size = lax.axis_size("gy")
    w_rows = key_matrix.shape[0]
    kv_cols = key_matrix.shape[1]
    kv_local = kv_cols // HEAD_SIZE
    group_cols = query_weight.shape[1] // kv_local
    gathered = lax.all_gather(tokens, "gx", axis=1, tiled=True)
    stacked = jnp.concatenate([key_matrix, value_matrix], axis=1)
    kv_pieces, arrived = ring_pieces(stacked)
    q_pieces = []
    for g in range(kv_local):
        own_block = query_weight[:, g * group_cols : (g + 1) * group_cols]
        held = lax.optimization_barrier((own_block, *arrived))
        got, arrived = ring_pieces(held[0])
        q_pieces.append(got)

    all_positions = layout_positions(pair_ids, tok_dev * size, tok_dev)
    own_index = lax.axis_index("gy")
    own_positions = lax.dynamic_slice_in_dim(all_positions, own_index * tok_dev, tok_dev, 0)
    own_pair = table_lookup(pair_ids, jnp.reshape(own_index, (1,)))[0]
    own = jnp.stack([own_pair, 2 * size - 1 - own_pair]).astype(jnp.int32)
    ids = lax.iota(jnp.int32, size)
    inverse = jnp.sum(jnp.where(pair_ids[None, :] == ids[:, None], ids[None, :], 0), axis=1)
    order = jnp.concatenate([2 * inverse, 2 * inverse[::-1] + 1]).astype(jnp.int32)
    half_size = HEAD_SIZE // 2
    frequency = jnp.exp(
        lax.iota(jnp.float32, half_size) * (-2.0 * math.log(rope_theta) / HEAD_SIZE)
    )
    angles = own_positions.astype(jnp.float32)[:, None] * frequency[None, :]
    cos_part, sin_part = jnp.cos(angles), jnp.sin(angles)
    cos_full = jnp.concatenate([cos_part, cos_part], axis=1)
    sin_full = jnp.concatenate([-sin_part, sin_part], axis=1)

    kv = project(gathered, kv_pieces, w_rows, jnp.concatenate([key_bias, value_offset_bias]))
    key_rows = apply_rotary(kv[:, :kv_cols].reshape(tok_dev, kv_local, HEAD_SIZE), own_positions)
    both = jnp.concatenate([key_rows.reshape(tok_dev, kv_cols), kv[:, kv_cols:]], axis=1)
    both = lax.all_gather(both.astype(jnp.bfloat16), "gy", axis=0, tiled=True)
    both = both.reshape(2 * size, half_len, 2, kv_local, HEAD_SIZE)
    outs = []
    for g in range(kv_local):
        cols = slice(g * group_cols, (g + 1) * group_cols)
        q = project(gathered, q_pieces[g], w_rows, query_bias[cols])
        k = both[:, :, 0, g]
        v = both[:, :, 1, g].transpose(0, 2, 1)
        outs.append(group_attention(order, own, q, cos_full, sin_full, k, v))
    return jnp.concatenate(outs, axis=1)


def solution(mesh):
    in_specs = (
        P("gy", "gx"),
        P(),
        P("gy", "gx"),
        P("gy", "gx"),
        P("gy", "gx"),
        P("gx"),
        P("gx"),
        P("gx"),
    )
    out_specs = P("gy", "gx")
    return jax.shard_map(
        on_device, mesh=mesh, in_specs=in_specs, out_specs=out_specs, check_vma=False
    )
```
